512 devices in a mesh: surf: 128 (over z, y, core), pair: 4 (over x).
Axes of the slice: x: 4, y: 4, z: 16, core: 2. Of those that a mesh axis runs over, the one named last changes fastest.
Arguments:
- left_panel: bfloat16 [1024, 4, 128, 192], P(('surf', 'pair')), may hold values from -0.5 to 0.5
- right_panel: bfloat16 [1024, 4, 128, 192], P(('surf', 'pair')), may hold values from -6 to 6
- inverse: bfloat16 [1024, 128, 128], P(('surf', 'pair')), may hold values from -0.5 to 0.5
- target: int32 [1024, 4, 4], P(('surf', 'pair')), may hold values from 0 to 2047, as said below
- blocks: float32 [2048, 192, 192], P(('surf', 'pair')), may hold values from -12 to 12
- weights: bfloat16 [2048, 192, 512], P('surf', None, 'pair'), may hold values from -0.109375 to 0.109375
Outputs:
- updated: float32 [2048, 192, 192], P(('surf', 'pair'))
- coarse_panel: float32 [24576, 512], P('surf', 'pair')
The draws below stay inside these ranges and needn't reach their ends.
Inputs may be any that keep to these rules, and one draw needn't show every extreme that they name: target[b, k, l] = target[b, l, k]. Pair block p lies on device p // 4 of the joined axes; the block of every term lies on a device with the same index along pair as the box's device, whose index along surf differs from the box's device's by at most 2 along the closed loop of 128 tiles. From the boxes of one device at most 8 unordered neighbour pairs (k <= l) go to any one tile, and every device sends exactly 8 to some tile in every draw.
All inputs are finite; a program needn't handle non-finite values.
Results may differ from the reference program's by a relative error of at most 0.0055.
Values may be sent and summed in bfloat16 or wider, within the bound.
A program may use at most 64 MiB of HBM per device.

```python
import jax
import jax.numpy as jnp
import numpy as np
from jax import lax

REDUNDANT = 128
SKEL = 192
NEIGH = 4
REACH = 2
BOX_DEV = 2
PAIR_DEV = 4
UNITS = 20
CAP = 8
NBOX = 1024
NPAIR = 2048
TILES = 128
TILE_PAIRS = 16
COLS = 512
N_SURF = 128
N_PAIR = 4


def pair_table():
    table = np.zeros((NEIGH, NEIGH), np.int32)
    counter = 0
    for first in range(NEIGH):
        for second in range(first, NEIGH):
            table[first, second] = counter
            table[second, first] = counter
            counter += 1
    return table


def draw_target(key, part):
    device_count = NBOX // BOX_DEV
    spots = 2 * REACH + 1
    slot_count = spots * CAP
    key_popular, key_hot, key_noise, key_order, key_block = jax.random.split(jax.random.fold_in(key, 7), 5)
    popular = jax.random.randint(key_popular, (device_count, spots), 0, 4)
    hottest = jax.random.randint(key_hot, (device_count,), 0, spots)
    slot_spot = jnp.arange(slot_count) // CAP
    bias = popular[:, slot_spot] * 4096 + (slot_spot[None, :] == hottest[:, None]).astype(jnp.int32) * 32768
    noise = jax.random.randint(key_noise, (device_count, slot_count), 0, 4096)
    scores = (bias + noise) * slot_count + jnp.arange(slot_count)[None, :]
    _, chosen = lax.top_k(scores, UNITS)
    order_keys = jax.random.randint(key_order, (device_count, UNITS), 0, 65536) * UNITS + jnp.arange(UNITS)[None, :]
    shuffle = jnp.argsort(order_keys, axis=1, stable=True)
    chosen = jnp.take_along_axis(chosen, shuffle, axis=1)
    offset = chosen // CAP - REACH
    device = jnp.arange(device_count)
    own_tile = device // N_PAIR
    pair_index = device % N_PAIR
    dest_tile = (own_tile[:, None] + offset + N_SURF) % N_SURF
    block_slot = jax.random.randint(key_block, (device_count, UNITS), 0, PAIR_DEV)
    unit_target = ((dest_tile * N_PAIR + pair_index[:, None]) * PAIR_DEV + block_slot).reshape(NBOX, UNITS // BOX_DEV)
    table = jnp.asarray(pair_table().reshape(-1))
    return unit_target[:, table].reshape(NBOX, NEIGH, NEIGH).astype(jnp.int32)


def shard_levels(stream_key, extent, shards, least, high):
    gain, own = 1.0, jax.random.fold_in(stream_key, 6)
    for axis_at, shards_of in shards:
        draws = jnp.exp(jax.random.uniform(jax.random.fold_in(own, axis_at), (shards_of,), jnp.float32, least / len(shards), high / len(shards)))
        gain = gain * jnp.repeat(draws, extent[axis_at] // shards_of).reshape([-1 if axis == axis_at else 1 for axis in range(len(extent))])
    return gain


def bell_draw(own_key, dims, deviation, limit, shards=(), dtype=jnp.bfloat16):
    entries = jax.random.normal(own_key, dims, jnp.float32) * deviation
    if len(shards) > 0:
        entries = shard_levels(own_key, dims, shards, -0.22, 0.18) * entries
    return jnp.clip(entries, min=-limit, max=limit).astype(dtype)


def setup_inputs(seed: int = 0) -> dict:
    seeds = jax.random.split(jax.random.key(seed), 7)
    left_panel = bell_draw(seeds[0], (NBOX, NEIGH, REDUNDANT, SKEL), REDUNDANT ** -0.5, 0.5, ((0, 512),))
    right_panel = bell_draw(seeds[1], (NBOX, NEIGH, REDUNDANT, SKEL), 1.0, 6.0, ((0, 512),))
    inverse = bell_draw(seeds[2], (NBOX, REDUNDANT, REDUNDANT), REDUNDANT ** -0.5, 0.5, ((0, 512),))
    target = draw_target(jax.random.fold_in(seeds[6], 71), 0)
    blocks = bell_draw(seeds[4], (NPAIR, SKEL, SKEL), 2.0, 12.0, ((0, 512),), jnp.float32)
    weights = bell_draw(seeds[5], (NPAIR, SKEL, COLS), (TILE_PAIRS * SKEL) ** -0.5, 0.109375, ((0, 128), (2, 4)))
    return dict(left_panel=left_panel, right_panel=right_panel, inverse=inverse, target=target, blocks=blocks, weights=weights)


def reference(left_panel, right_panel, inverse, target, blocks, weights):
    lower = (jnp.arange(NEIGH)[:, None] > jnp.arange(NEIGH)[None, :])[:, :, None, None]

    def eliminate(running, inputs):
        left_box, right_box, inverse_box, target_box = inputs
        solved = jnp.einsum('ij,kjc->kic', inverse_box.astype(jnp.float32), right_box.astype(jnp.float32)).astype(jnp.bfloat16)
        solved = lax.optimization_barrier(solved).astype(jnp.float32)
        products = jnp.einsum('kri,lrj->klij', left_box.astype(jnp.float32), solved).astype(jnp.bfloat16)
        products = lax.optimization_barrier(products).astype(jnp.float32)
        chosen = jnp.where(lower, jnp.swapaxes(products, 2, 3), products)
        running = running.at[target_box.reshape(-1).astype(jnp.int32)].add(-chosen.reshape(-1, SKEL, SKEL))
        return running, None

    updated, _ = lax.scan(eliminate, blocks, (left_panel, right_panel, inverse, target))
    rounded = lax.optimization_barrier(updated.astype(jnp.bfloat16)).astype(jnp.float32)
    tiled = rounded.reshape(TILES, TILE_PAIRS, SKEL, SKEL)
    tiled_weights = weights.astype(jnp.float32).reshape(TILES, TILE_PAIRS, SKEL, COLS)
    coarse_panel = jnp.einsum('tpij,tpjc->tic', tiled, tiled_weights).reshape(TILES * SKEL, COLS)
    return updated, coarse_panel
```

```python
import functools

import jax
import jax.numpy as jnp
from jax import lax
from jax.experimental import pallas as pl
from jax.experimental.pallas import tpu as pltpu
from jax.sharding import PartitionSpec as P

MESH = pl.DeviceIdType.MESH
REACH = 2
SPOTS = 2 * REACH + 1
CHUNKS = 3
RELAY, PARTNER, NEAR, FAR = 0, 1, 2, 3
SPOT_OF = {RELAY: 0, PARTNER: 1, NEAR: 3, FAR: 4}
OWN_SPOT = 2


def kernel(
    n_surf, n_pair, target, left, right, inverse, blocks, weights, updated, coarse,
    left_v, right_v, inverse_v, blocks_v, rows_a, cols_b, acc, index, pieces, arrived,
    weights_v, rounded, updated_v, part, part_in, coarse_v,
    load_sem, send_sem, recv_sem, wsend_sem, wrecv_sem, psend_sem, precv_sem, out_sem,
):
    boxes, neighbours, skeleton, redundant = left.shape
    local = blocks.shape[0]
    rows = skeleton // CHUNKS
    half = rows // 2
    packed = rows + half
    surf = lax.axis_index("surf")
    pair = lax.axis_index("pair")
    out = 2 * lax.rem(surf, 2) - 1

    def tile(offset):
        return lax.rem(surf + out * offset + n_surf, n_surf)

    def across(offset):
        return lax.rem(pair + offset, n_pair)

    barrier = pltpu.get_barrier_semaphore()
    for offset in (-1, 1, -2, 2):
        pl.semaphore_signal(barrier, inc=1, device_id=(tile(offset), pair), device_id_type=MESH)
    for offset in range(1, n_pair):
        pl.semaphore_signal(barrier, inc=1, device_id=(surf, across(offset)), device_id_type=MESH)

    loads = [
        pltpu.make_async_copy(source, into, load_sem.at[at])
        for at, (source, into) in enumerate(
            [
                (inverse, inverse_v),
                (right, right_v),
                (left, left_v),
                (weights.at[pl.ds(pair * local, local)], weights_v.at[0]),
                (blocks, blocks_v),
            ]
        )
    ]
    for load in loads:
        load.start()

    units = [(b, k, l) for b in range(boxes) for k in range(neighbours) for l in range(k, neighbours)]
    count = len(units)
    where_to = []
    for b, k, l in units:
        block = target[b, k, l]
        ahead = lax.rem(block // (local * n_pair) - surf + n_surf, n_surf)
        ahead = jnp.where(ahead <= REACH, ahead, ahead - n_surf)
        where_to.append((ahead * out + REACH) * local + lax.rem(block, local))
    for u in range(count):
        before = jnp.int32(count)
        for v in range(u):
            before = jnp.where(where_to[v] == where_to[u], v, before)
        index[u] = before
    for d in range(SPOTS * local):
        last = jnp.int32(count)
        for u in range(count):
            last = jnp.where(where_to[u] == d, u, last)
        index[count + d] = last

    acc[count] = jnp.zeros(acc.shape[1:], jnp.float32)

    pl.semaphore_wait(barrier, 3 + n_pair)

    wcopies = []
    for offset in (2, 1, 3):
        slot = n_pair - offset
        copy = pltpu.make_async_remote_copy(
            src_ref=weights.at[pl.ds(across(offset) * local, local)],
            dst_ref=weights_v.at[slot],
            send_sem=wsend_sem.at[slot - 1],
            recv_sem=wrecv_sem.at[slot - 1],
            device_id=(surf, across(offset)),
            device_id_type=MESH,
        )
        copy.start()
        wcopies.append(copy)

    for load in loads[:3]:
        load.wait()

    for b in range(boxes):
        solved = lax.dot_general(
            right_v[b].reshape(neighbours * skeleton, redundant),
            inverse_v[b],
            (((1,), (1,)), ((), ())),
            preferred_element_type=jnp.float32,
        ).astype(jnp.bfloat16)
        for k in range(neighbours):
            mine = solved[k * skeleton : (k + 1) * skeleton]
            panel = left_v[b, k]
            rows_a[b, k, :, :redundant] = panel
            rows_a[b, k, :, redundant:] = mine
            both = jnp.concatenate([mine, panel], axis=1)
            both = jnp.concatenate([both, both[redundant:]], axis=0)
            cols_b[b, k] = both.T

    lanes = lax.broadcasted_iota(jnp.int32, (half, 128), 1)
    for u, (b, k, l) in enumerate(units):
        if k == l:
            unit = jnp.dot(
                rows_a[b, k, :, :redundant], cols_b[b, l, :redundant], preferred_element_type=jnp.float32
            )
        else:
            unit = jnp.dot(rows_a[b, k], cols_b[b, l], preferred_element_type=jnp.float32)
        before = index[u]
        for r in range(CHUNKS):
            top = r * rows
            at = r * packed
            acc[u, at : at + rows] = unit[top : top + rows, :128] + acc[before, at : at + rows]
            tail = jnp.where(lanes < 64, unit[top : top + half, 128:], unit[top + half : top + rows, 128:])
            acc[u, at + rows : at + packed] = tail + acc[before, at + rows : at + packed]

    def piece_of(spot, slot, r):
        return acc[index[count + spot * local + slot], r * packed : (r + 1) * packed]

    to = {RELAY: -1, PARTNER: -1, NEAR: 1, FAR: 2}

    def send(kind, r):
        copy = pltpu.make_async_remote_copy(
            src_ref=pieces.at[kind, r],
            dst_ref=arrived.at[kind, r],
            send_sem=send_sem.at[kind, r],
            recv_sem=recv_sem.at[kind, r],
            device_id=(tile(to[kind]), pair),
            device_id_type=MESH,
        )
        copy.start()
        return copy

    copies = {}
    for r in range(CHUNKS):
        for kind in (RELAY, FAR, PARTNER):
            for slot in range(local):
                pieces[kind, r, slot] = piece_of(SPOT_OF[kind], slot, r).astype(jnp.bfloat16)
            copies[kind, r] = send(kind, r)
    for r in range(CHUNKS):
        copies[RELAY, r].wait_recv()
        for slot in range(local):
            joined = piece_of(SPOT_OF[NEAR], slot, r) + arrived[RELAY, r, slot].astype(jnp.float32)
            pieces[NEAR, r, slot] = joined.astype(jnp.bfloat16)
        copies[NEAR, r] = send(NEAR, r)

    loads[3].wait()
    loads[4].wait()
    pcopies = []
    outs = []
    own = []
    for r in range(CHUNKS):
        top = r * rows
        for kind in (PARTNER, FAR, NEAR):
            copies[kind, r].wait_recv()
        for slot in range(local):
            total = piece_of(OWN_SPOT, slot, r)
            for kind in (PARTNER, FAR, NEAR):
                total = total + arrived[kind, r, slot].astype(jnp.float32)
            tail = total[rows:]
            tail = jnp.concatenate([tail, pltpu.roll(tail, 64, axis=1)], axis=0)[:, :64]
            main = blocks_v[slot, top : top + rows, :128] - total[:rows]
            tail = blocks_v[slot, top : top + rows, 128:] - tail
            updated_v[slot, top : top + rows, :128] = main
            updated_v[slot, top : top + rows, 128:] = tail
            rounded[slot, :, :128] = main.astype(jnp.bfloat16)
            rounded[slot, :, 128:] = tail.astype(jnp.bfloat16)
        copy = pltpu.make_async_copy(
            updated_v.at[:, pl.ds(top, rows)], updated.at[:, pl.ds(top, rows)], out_sem.at[r]
        )
        copy.start()
        outs.append(copy)
        if r == 0:
            for copy in wcopies:
                copy.wait_recv()

        def panel_of(first, second):
            total = None
            for slot in range(local):
                both = jnp.concatenate([weights_v[first, slot], weights_v[second, slot]], axis=1)
                term = jnp.dot(rounded[slot], both, preferred_element_type=jnp.float32)
                total = term if total is None else total + term
            return total

        def send_part(offset, value):
            part[offset - 1, r] = value.astype(jnp.bfloat16)
            slot = n_pair - offset - 1
            copy = pltpu.make_async_remote_copy(
                src_ref=part.at[offset - 1, r],
                dst_ref=part_in.at[slot, r],
                send_sem=psend_sem.at[slot, r],
                recv_sem=precv_sem.at[slot, r],
                device_id=(surf, across(offset)),
                device_id_type=MESH,
            )
            copy.start()
            pcopies.append((r, copy))

        panel = panel_of(2, 1)
        send_part(2, panel[:, :128])
        send_part(1, panel[:, 128:])
        panel = panel_of(3, 0)
        send_part(3, panel[:, :128])
        coarse_v[top : top + rows] = panel[:, 128:]

    for r in range(CHUNKS):
        top = r * rows
        for at, copy in pcopies:
            if at == r:
                copy.wait_recv()
        total = coarse_v[top : top + rows]
        for slot in range(n_pair - 1):
            total = total + part_in[slot, r].astype(jnp.float32)
        coarse_v[top : top + rows] = total
    copy = pltpu.make_async_copy(coarse_v, coarse, out_sem.at[CHUNKS])
    copy.start()
    outs.append(copy)
    for copy in wcopies:
        copy.wait_send()
    for copy in copies.values():
        copy.wait_send()
    for _, copy in pcopies:
        copy.wait_send()
    for copy in outs:
        copy.wait()


def body(left, right, inverse, target, blocks, weights):
    n_surf = lax.axis_size("surf")
    n_pair = lax.axis_size("pair")
    boxes, neighbours, redundant, skeleton = left.shape
    local = blocks.shape[0]
    columns = weights.shape[2]
    packed = skeleton * 3 // 2 // CHUNKS
    rows = skeleton // CHUNKS
    count = boxes * neighbours * (neighbours + 1) // 2
    bf16, f32 = jnp.bfloat16, jnp.float32
    anywhere = pl.BlockSpec(memory_space=pl.ANY)
    dma = pltpu.SemaphoreType.DMA
    return pl.pallas_call(
        functools.partial(kernel, n_surf, n_pair),
        name="eliminate",
        out_shape=(
            jax.ShapeDtypeStruct(blocks.shape, f32),
            jax.ShapeDtypeStruct((skeleton, columns), f32),
        ),
        in_specs=[pl.BlockSpec(memory_space=pltpu.SMEM)] + [anywhere] * 5,
        out_specs=(anywhere, anywhere),
        scratch_shapes=[
            pltpu.VMEM((boxes, neighbours, skeleton, redundant), bf16),
            pltpu.VMEM((boxes, neighbours, skeleton, redundant), bf16),
            pltpu.VMEM(inverse.shape, bf16),
            pltpu.VMEM(blocks.shape, f32),
            pltpu.VMEM((boxes, neighbours, skeleton, 2 * redundant), bf16),
            pltpu.VMEM((boxes, neighbours, 2 * redundant, 256), bf16),
            pltpu.VMEM((count + 1, CHUNKS * packed, 128), f32),
            pltpu.SMEM((count + SPOTS * local,), jnp.int32),
            pltpu.VMEM((4, CHUNKS, local, packed, 128), bf16),
            pltpu.VMEM((4, CHUNKS, local, packed, 128), bf16),
            pltpu.VMEM((n_pair, local, skeleton, columns), bf16),
            pltpu.VMEM((local, rows, skeleton), bf16),
            pltpu.VMEM(blocks.shape, f32),
            pltpu.VMEM((n_pair - 1, CHUNKS, rows, columns), bf16),
            pltpu.VMEM((n_pair - 1, CHUNKS, rows, columns), bf16),
            pltpu.VMEM((skeleton, columns), f32),
            dma((5,)),
            dma((4, CHUNKS)),
            dma((4, CHUNKS)),
            dma((n_pair - 1,)),
            dma((n_pair - 1,)),
            dma((n_pair - 1, CHUNKS)),
            dma((n_pair - 1, CHUNKS)),
            dma((CHUNKS + 1,)),
        ],
        compiler_params=pltpu.CompilerParams(collective_id=0, has_side_effects=True),
    )(target, jnp.swapaxes(left, 2, 3), jnp.swapaxes(right, 2, 3), inverse, blocks, weights)


def solution(mesh):
    in_specs = (
        P(("surf", "pair"), None, None, None),
        P(("surf", "pair"), None, None, None),
        P(("surf", "pair"), None, None),
        P(("surf", "pair"), None, None),
        P(("surf", "pair"), None, None),
        P("surf", None, "pair"),
    )
    out_specs = (P(("surf", "pair"), None, None), P("surf", "pair"))
    return jax.shard_map(body, mesh=mesh, in_specs=in_specs, out_specs=out_specs, check_vma=False)
```

```python
import functools

import jax
import jax.numpy as jnp
from jax import lax
from jax.experimental import pallas as pl
from jax.experimental.pallas import tpu as pltpu
from jax.sharding import PartitionSpec as P

MESH = pl.DeviceIdType.MESH
REACH = 2
SPOTS = 2 * REACH + 1
CHUNKS = 3
RELAY, PARTNER, NEAR, FAR = 0, 1, 2, 3
SPOT_OF = {RELAY: 0, PARTNER: 1, NEAR: 3, FAR: 4}
OWN_SPOT = 2


def kernel(
    n_surf, n_pair, target, left, right, inverse, blocks, weights, updated, coarse,
    target_s, left_v, right_v, inverse_v, blocks_v, rows_a, cols_b, acc, index, pieces, arrived,
    weights_v, rounded, part, part_in,
    load_sem, send_sem, recv_sem, wsend_sem, wrecv_sem, psend_sem, precv_sem,
):
    boxes, neighbours, skeleton, redundant = left.shape
    local = blocks.shape[0]
    rows = skeleton // CHUNKS
    half = rows // 2
    packed = rows + half
    surf = lax.axis_index("surf")
    pair = lax.axis_index("pair")
    out = 2 * lax.rem(surf, 2) - 1

    def tile(offset):
        return lax.rem(surf + out * offset + n_surf, n_surf)

    def across(offset):
        return lax.rem(pair + offset, n_pair)

    barrier = pltpu.get_barrier_semaphore()
    late = jnp.maximum(REACH - surf, 0)

    def greet(closing):
        for offset in range(-REACH, REACH + 1):
            if offset != 0:
                peer = surf + offset
                closes = jnp.logical_or(peer < 0, peer >= n_surf)

                @pl.when(closes if closing else jnp.logical_not(closes))
                def _():
                    there = lax.rem(peer + n_surf, n_surf)
                    pl.semaphore_signal(barrier, inc=1, device_id=(there, pair), device_id_type=MESH)

    for offset in range(1, n_pair):
        pl.semaphore_signal(barrier, inc=1, device_id=(surf, across(offset)), device_id_type=MESH)
    greet(False)

    loads = [
        pltpu.make_async_copy(source, into, load_sem.at[at])
        for at, (source, into) in enumerate(
            [
                (target, target_s),
                (inverse, inverse_v),
                (right, right_v),
                (left, left_v),
                (weights.at[pl.ds(pair * local, local)], weights_v.at[0]),
                (blocks, blocks_v),
            ]
        )
    ]
    for load in loads:
        load.start()

    for load in loads[:4]:
        load.wait()

    units = [(b, k, l) for b in range(boxes) for k in range(neighbours) for l in range(k, neighbours)]
    count = len(units)
    where_to = []
    for b, k, l in units:
        block = target_s[b, k, l]
        ahead = lax.rem(block // (local * n_pair) - surf + n_surf, n_surf)
        ahead = jnp.where(ahead <= REACH, ahead, ahead - n_surf)
        where_to.append((ahead * out + REACH) * local + lax.rem(block, local))
    for u in range(count):
        before = jnp.int32(count)
        for v in range(u):
            before = jnp.where(where_to[v] == where_to[u], v, before)
        index[u] = before
    for d in range(SPOTS * local):
        last = jnp.int32(count)
        for u in range(count):
            last = jnp.where(where_to[u] == d, u, last)
        index[count + d] = last

    acc[count] = jnp.zeros(acc.shape[1:], jnp.float32)

    for b in range(boxes):
        solved = lax.dot_general(
            right_v[b].reshape(neighbours * skeleton, redundant),
            inverse_v[b],
            (((1,), (1,)), ((), ())),
            preferred_element_type=jnp.float32,
        ).astype(jnp.bfloat16)
        for k in range(neighbours):
            mine = solved[k * skeleton : (k + 1) * skeleton]
            panel = left_v[b, k]
            rows_a[b, k, :, :redundant] = panel
            rows_a[b, k, :, redundant:] = mine
            both = jnp.concatenate([mine, panel], axis=1)
            both = jnp.concatenate([both, both[redundant:]], axis=0)
            cols_b[b, k] = both.T

    lanes = lax.broadcasted_iota(jnp.int32, (half, 128), 1)
    for u, (b, k, l) in enumerate(units):
        if k == l:
            unit = jnp.dot(
                rows_a[b, k, :, :redundant], cols_b[b, l, :redundant], preferred_element_type=jnp.float32
            )
        else:
            unit = jnp.dot(rows_a[b, k], cols_b[b, l], preferred_element_type=jnp.float32)
        before = index[u]
        for r in range(CHUNKS):
            top = r * rows
            at = r * packed
            acc[u, at : at + rows] = unit[top : top + rows, :128] + acc[before, at : at + rows]
            tail = jnp.where(lanes < 64, unit[top : top + half, 128:], unit[top + half : top + rows, 128:])
            acc[u, at + rows : at + packed] = tail + acc[before, at + rows : at + packed]

    pl.semaphore_wait(barrier, 2 * REACH + n_pair - 1 - late)
    greet(True)

    wcopies = []
    for offset in (2, 1, 3):
        slot = n_pair - offset
        copy = pltpu.make_async_remote_copy(
            src_ref=weights.at[pl.ds(across(offset) * local, local)],
            dst_ref=weights_v.at[slot],
            send_sem=wsend_sem.at[slot - 1],
            recv_sem=wrecv_sem.at[slot - 1],
            device_id=(surf, across(offset)),
            device_id_type=MESH,
        )
        copy.start()
        wcopies.append(copy)

    def piece_of(spot, slot, r):
        return acc[index[count + spot * local + slot], r * packed : (r + 1) * packed]

    to = {RELAY: -1, PARTNER: -1, NEAR: 1, FAR: 2}

    def send(kind, r):
        copy = pltpu.make_async_remote_copy(
            src_ref=pieces.at[kind, r],
            dst_ref=arrived.at[kind, r],
            send_sem=send_sem.at[kind, r],
            recv_sem=recv_sem.at[kind, r],
            device_id=(tile(to[kind]), pair),
            device_id_type=MESH,
        )
        copy.start()
        return copy

    copies = {}
    for kind in (RELAY, PARTNER, FAR):
        if kind == FAR:
            @pl.when(surf == 0)
            def _():
                pl.semaphore_wait(barrier, REACH)

        for r in range(CHUNKS):
            for slot in range(local):
                pieces[kind, r, slot] = piece_of(SPOT_OF[kind], slot, r).astype(jnp.bfloat16)
            copies[kind, r] = send(kind, r)
    for r in range(CHUNKS):
        copies[RELAY, r].wait_recv()
        for slot in range(local):
            joined = piece_of(SPOT_OF[NEAR], slot, r) + arrived[RELAY, r, slot].astype(jnp.float32)
            pieces[NEAR, r, slot] = joined.astype(jnp.bfloat16)
        copies[NEAR, r] = send(NEAR, r)

    loads[4].wait()
    loads[5].wait()
    pcopies = []
    own = []
    for r in range(CHUNKS):
        top = r * rows
        for kind in (PARTNER, FAR, NEAR):
            copies[kind, r].wait_recv()
        for slot in range(local):
            total = piece_of(OWN_SPOT, slot, r)
            for kind in (PARTNER, FAR, NEAR):
                total = total + arrived[kind, r, slot].astype(jnp.float32)
            tail = total[rows:]
            tail = jnp.concatenate([tail, pltpu.roll(tail, 64, axis=1)], axis=0)[:, :64]
            main = blocks_v[slot, top : top + rows, :128] - total[:rows]
            tail = blocks_v[slot, top : top + rows, 128:] - tail
            updated[slot, top : top + rows, :128] = main
            updated[slot, top : top + rows, 128:] = tail
            rounded[slot, :, :128] = main.astype(jnp.bfloat16)
            rounded[slot, :, 128:] = tail.astype(jnp.bfloat16)
        if r == 0:
            for copy in wcopies:
                copy.wait_recv()

        def panel_of(first, second):
            total = None
            for slot in range(local):
                both = jnp.concatenate([weights_v[first, slot], weights_v[second, slot]], axis=1)
                term = jnp.dot(rounded[slot], both, preferred_element_type=jnp.float32)
                total = term if total is None else total + term
            return total

        def send_part(offset, value):
            part[offset - 1, r] = value.astype(jnp.bfloat16)
            slot = n_pair - offset - 1
            copy = pltpu.make_async_remote_copy(
                src_ref=part.at[offset - 1, r],
                dst_ref=part_in.at[slot, r],
                send_sem=psend_sem.at[slot, r],
                recv_sem=precv_sem.at[slot, r],
                device_id=(surf, across(offset)),
                device_id_type=MESH,
            )
            copy.start()
            pcopies.append((r, copy))

        panel = panel_of(2, 1)
        send_part(2, panel[:, :128])
        send_part(1, panel[:, 128:])
        panel = panel_of(3, 0)
        send_part(3, panel[:, :128])
        coarse[top : top + rows] = panel[:, 128:]

    for r in range(CHUNKS):
        top = r * rows
        for at, copy in pcopies:
            if at == r:
                copy.wait_recv()
        total = coarse[top : top + rows]
        for slot in range(n_pair - 1):
            total = total + part_in[slot, r].astype(jnp.float32)
        coarse[top : top + rows] = total
    @pl.when(surf == 1)
    def _():
        pl.semaphore_wait(barrier, 1)

    for copy in wcopies:
        copy.wait_send()
    for copy in copies.values():
        copy.wait_send()
    for _, copy in pcopies:
        copy.wait_send()


def body(left, right, inverse, target, blocks, weights):
    n_surf = lax.axis_size("surf")
    n_pair = lax.axis_size("pair")
    boxes, neighbours, redundant, skeleton = left.shape
    local = blocks.shape[0]
    columns = weights.shape[2]
    packed = skeleton * 3 // 2 // CHUNKS
    rows = skeleton // CHUNKS
    count = boxes * neighbours * (neighbours + 1) // 2
    bf16, f32 = jnp.bfloat16, jnp.float32
    anywhere = pl.BlockSpec(memory_space=pl.ANY)
    on_chip = pl.BlockSpec(memory_space=pltpu.VMEM)
    dma = pltpu.SemaphoreType.DMA
    return pl.pallas_call(
        functools.partial(kernel, n_surf, n_pair),
        name="eliminate",
        out_shape=(
            pltpu.VMEM(blocks.shape, f32),
            pltpu.VMEM((skeleton, columns), f32),
        ),
        in_specs=[anywhere] * 6,
        out_specs=(on_chip, on_chip),
        scratch_shapes=[
            pltpu.SMEM((boxes, neighbours, neighbours), jnp.int32),
            pltpu.VMEM((boxes, neighbours, skeleton, redundant), bf16),
            pltpu.VMEM((boxes, neighbours, skeleton, redundant), bf16),
            pltpu.VMEM(inverse.shape, bf16),
            pltpu.VMEM(blocks.shape, f32),
            pltpu.VMEM((boxes, neighbours, skeleton, 2 * redundant), bf16),
            pltpu.VMEM((boxes, neighbours, 2 * redundant, 256), bf16),
            pltpu.VMEM((count + 1, CHUNKS * packed, 128), f32),
            pltpu.SMEM((count + SPOTS * local,), jnp.int32),
            pltpu.VMEM((4, CHUNKS, local, packed, 128), bf16),
            pltpu.VMEM((4, CHUNKS, local, packed, 128), bf16),
            pltpu.VMEM((n_pair, local, skeleton, columns), bf16),
            pltpu.VMEM((local, rows, skeleton), bf16),
            pltpu.VMEM((n_pair - 1, CHUNKS, rows, columns), bf16),
            pltpu.VMEM((n_pair - 1, CHUNKS, rows, columns), bf16),
            dma((6,)),
            dma((4, CHUNKS)),
            dma((4, CHUNKS)),
            dma((n_pair - 1,)),
            dma((n_pair - 1,)),
            dma((n_pair - 1, CHUNKS)),
            dma((n_pair - 1, CHUNKS)),
        ],
        compiler_params=pltpu.CompilerParams(collective_id=0, has_side_effects=True, vmem_limit_bytes=66048000),
    )(target, jnp.swapaxes(left, 2, 3), jnp.swapaxes(right, 2, 3), inverse, blocks, weights)


def solution(mesh):
    in_specs = (
        P(("surf", "pair"), None, None, None),
        P(("surf", "pair"), None, None, None),
        P(("surf", "pair"), None, None),
        P(("surf", "pair"), None, None),
        P(("surf", "pair"), None, None),
        P("surf", None, "pair"),
    )
    out_specs = (P(("surf", "pair"), None, None), P("surf", "pair"))
    return jax.shard_map(body, mesh=mesh, in_specs=in_specs, out_specs=out_specs, check_vma=False)
```

```python
import functools

import jax
import jax.numpy as jnp
from jax import lax
from jax.experimental import pallas as pl
from jax.experimental.pallas import tpu as pltpu
from jax.sharding import PartitionSpec as P

MESH = pl.DeviceIdType.MESH
REACH = 2
SPOTS = 2 * REACH + 1
CHUNKS = 3
VMEM = 66048000
RELAY, PARTNER, NEAR, FAR = 0, 1, 2, 3
SPOT_OF = {RELAY: 0, PARTNER: 1, NEAR: 3, FAR: 4}
OWN_SPOT = 2


def kernel(
    n_surf, n_pair, target, left, right, inverse, blocks, weights, updated, coarse,
    target_s, left_v, right_v, inverse_v, blocks_v, rows_a, cols_b, acc, index, pieces, arrived,
    weights_own, weights_in, rounded, part, part_in,
    load_sem, send_sem, partner_sem, recv_sem, wsend_sem, wrecv_sem, psend_sem, precv_sem,
):
    boxes, neighbours, skeleton, redundant = left.shape
    local = blocks.shape[0]
    rows = skeleton // CHUNKS
    half = rows // 2
    packed = rows + half
    surf = lax.axis_index("surf")
    pair = lax.axis_index("pair")
    out = 2 * lax.rem(surf, 2) - 1

    def tile(offset):
        return lax.rem(surf + out * offset + n_surf, n_surf)

    def across(offset):
        return lax.rem(pair + offset, n_pair)

    loads = [
        pltpu.make_async_copy(source, into, load_sem.at[at])
        for at, (source, into) in enumerate(
            [
                (target, target_s),
                (inverse, inverse_v),
                (right, right_v),
                (left, left_v),
                (weights.at[pl.ds(pair * local, local)], weights_own),
                (blocks, blocks_v),
            ]
        )
    ]
    for load in loads:
        load.start()

    barrier = pltpu.get_barrier_semaphore()
    late = jnp.maximum(REACH - surf, 0)

    def greet(closing):
        for offset in range(-REACH, REACH + 1):
            if offset != 0:
                peer = surf + offset
                closes = jnp.logical_or(peer < 0, peer >= n_surf)

                @pl.when(closes if closing else jnp.logical_not(closes))
                def _():
                    there = lax.rem(peer + n_surf, n_surf)
                    pl.semaphore_signal(barrier, inc=1, device_id=(there, pair), device_id_type=MESH)

    for offset in range(1, n_pair):
        pl.semaphore_signal(barrier, inc=1, device_id=(surf, across(offset)), device_id_type=MESH)
    greet(False)

    for load in loads[:4]:
        load.wait()

    units = [(b, k, l) for b in range(boxes) for k in range(neighbours) for l in range(k, neighbours)]
    count = len(units)
    where_to = []
    for b, k, l in units:
        block = target_s[b, k, l]
        ahead = lax.rem(block // (local * n_pair) - surf + n_surf, n_surf)
        ahead = jnp.where(ahead <= REACH, ahead, ahead - n_surf)
        where_to.append((ahead * out + REACH) * local + lax.rem(block, local))
    for u in range(count):
        before = jnp.int32(count)
        for v in range(u):
            before = jnp.where(where_to[v] == where_to[u], v, before)
        index[u] = before
    for d in range(SPOTS * local):
        last = jnp.int32(count)
        for u in range(count):
            last = jnp.where(where_to[u] == d, u, last)
        index[count + d] = last

    acc[count] = jnp.zeros(acc.shape[1:], jnp.float32)

    for b in range(boxes):
        solved = lax.dot_general(
            right_v[b].reshape(neighbours * skeleton, redundant),
            inverse_v[b],
            (((1,), (1,)), ((), ())),
            preferred_element_type=jnp.float32,
        ).astype(jnp.bfloat16)
        for k in range(neighbours):
            mine = solved[k * skeleton : (k + 1) * skeleton]
            panel = left_v[b, k]
            rows_a[b, k, :, :redundant] = panel
            rows_a[b, k, :, redundant:] = mine
            both = jnp.concatenate([mine, panel], axis=1)
            both = jnp.concatenate([both, both[redundant:]], axis=0)
            cols_b[b, k] = both.T

    lanes = lax.broadcasted_iota(jnp.int32, (half, 128), 1)
    for u, (b, k, l) in enumerate(units):
        if k == l:
            unit = jnp.dot(
                rows_a[b, k, :, :redundant], cols_b[b, l, :redundant], preferred_element_type=jnp.float32
            )
        else:
            unit = jnp.dot(rows_a[b, k], cols_b[b, l], preferred_element_type=jnp.float32)
        before = index[u]
        for r in range(CHUNKS):
            top = r * rows
            at = r * packed
            acc[u, at : at + rows] = unit[top : top + rows, :128] + acc[before, at : at + rows]
            tail = jnp.where(lanes < 64, unit[top : top + half, 128:], unit[top + half : top + rows, 128:])
            acc[u, at + rows : at + packed] = tail + acc[before, at + rows : at + packed]

    pl.semaphore_wait(barrier, 2 * REACH + n_pair - 1 - late)
    greet(True)

    for offset in (2, 1, 3):
        slot = n_pair - offset
        copy = pltpu.make_async_remote_copy(
            src_ref=weights.at[pl.ds(across(offset) * local, local)],
            dst_ref=weights_in.at[pl.ds((slot - 1) * local, local)],
            send_sem=wsend_sem,
            recv_sem=wrecv_sem,
            device_id=(surf, across(offset)),
            device_id_type=MESH,
        )
        copy.start()

    def piece_of(spot, slot, r):
        return acc[index[count + spot * local + slot], r * packed : (r + 1) * packed]

    to = {RELAY: -1, PARTNER: -1, NEAR: 1, FAR: 2}

    def all_sent(source, into, sem):
        pltpu.make_async_remote_copy(
            src_ref=source, dst_ref=into, send_sem=sem, recv_sem=sem, device_id=(surf, across(1)), device_id_type=MESH
        ).wait_send()

    def all_in(source, into, sem):
        pltpu.make_async_remote_copy(
            src_ref=source, dst_ref=into, send_sem=sem, recv_sem=sem, device_id=(surf, across(1)), device_id_type=MESH
        ).wait_recv()

    def send(kind, r):
        copy = pltpu.make_async_remote_copy(
            src_ref=pieces.at[kind, r],
            dst_ref=arrived.at[kind, r],
            send_sem=send_sem,
            recv_sem=partner_sem if kind == PARTNER else recv_sem.at[kind, r],
            device_id=(tile(to[kind]), pair),
            device_id_type=MESH,
        )
        copy.start()
        return copy

    copies = {}
    for kind in (RELAY, PARTNER, FAR):
        if kind == FAR:
            @pl.when(surf == 0)
            def _():
                pl.semaphore_wait(barrier, REACH)

        for r in range(CHUNKS):
            for slot in range(local):
                pieces[kind, r, slot] = piece_of(SPOT_OF[kind], slot, r).astype(jnp.bfloat16)
            copies[kind, r] = send(kind, r)
    for r in range(CHUNKS):
        copies[RELAY, r].wait_recv()
        for slot in range(local):
            joined = piece_of(SPOT_OF[NEAR], slot, r) + arrived[RELAY, r, slot].astype(jnp.float32)
            pieces[NEAR, r, slot] = joined.astype(jnp.bfloat16)
        copies[NEAR, r] = send(NEAR, r)

    loads[4].wait()
    loads[5].wait()
    own = []
    for r in range(CHUNKS):
        top = r * rows
        if r == 0:
            all_in(pieces.at[PARTNER], arrived.at[PARTNER], partner_sem)
        for kind in (FAR, NEAR):
            copies[kind, r].wait_recv()
        for slot in range(local):
            total = piece_of(OWN_SPOT, slot, r)
            for kind in (PARTNER, FAR, NEAR):
                total = total + arrived[kind, r, slot].astype(jnp.float32)
            tail = total[rows:]
            tail = jnp.concatenate([tail, pltpu.roll(tail, 64, axis=1)], axis=0)[:, :64]
            main = blocks_v[slot, top : top + rows, :128] - total[:rows]
            tail = blocks_v[slot, top : top + rows, 128:] - tail
            updated[slot, top : top + rows, :128] = main
            updated[slot, top : top + rows, 128:] = tail
            rounded[slot, :, :128] = main.astype(jnp.bfloat16)
            rounded[slot, :, 128:] = tail.astype(jnp.bfloat16)
        if r == 0:
            all_in(weights.at[pl.ds(0, (n_pair - 1) * local)], weights_in, wrecv_sem)

        def weights_of(offset, slot):
            return weights_own[slot] if offset == 0 else weights_in[(offset - 1) * local + slot]

        def panel_of(first, second):
            total = None
            for slot in range(local):
                both = jnp.concatenate([weights_of(first, slot), weights_of(second, slot)], axis=1)
                term = jnp.dot(rounded[slot], both, preferred_element_type=jnp.float32)
                total = term if total is None else total + term
            return total

        def send_part(offset, value):
            part[offset - 1, r] = value.astype(jnp.bfloat16)
            slot = n_pair - offset - 1
            copy = pltpu.make_async_remote_copy(
                src_ref=part.at[offset - 1, r],
                dst_ref=part_in.at[slot, r],
                send_sem=psend_sem,
                recv_sem=precv_sem,
                device_id=(surf, across(offset)),
                device_id_type=MESH,
            )
            copy.start()

        panel = panel_of(2, 1)
        send_part(2, panel[:, :128])
        send_part(1, panel[:, 128:])
        panel = panel_of(3, 0)
        send_part(3, panel[:, :128])
        coarse[top : top + rows] = panel[:, 128:]

    all_in(part, part_in, precv_sem)
    for r in range(CHUNKS):
        top = r * rows
        total = coarse[top : top + rows]
        for slot in range(n_pair - 1):
            total = total + part_in[slot, r].astype(jnp.float32)
        coarse[top : top + rows] = total

    @pl.when(surf == 1)
    def _():
        pl.semaphore_wait(barrier, 1)

    all_sent(weights.at[pl.ds(0, (n_pair - 1) * local)], weights_in, wsend_sem)
    all_sent(pieces, arrived, send_sem)
    all_sent(part, part_in, psend_sem)


def store(updated, coarse, updated_out, coarse_out, sem):
    copies = [
        pltpu.make_async_copy(updated, updated_out, sem.at[0]),
        pltpu.make_async_copy(coarse, coarse_out, sem.at[1]),
    ]
    for copy in copies:
        copy.start()
    for copy in copies:
        copy.wait()


def body(left, right, inverse, target, blocks, weights):
    n_surf = lax.axis_size("surf")
    n_pair = lax.axis_size("pair")
    boxes, neighbours, redundant, skeleton = left.shape
    local = blocks.shape[0]
    columns = weights.shape[2]
    packed = skeleton * 3 // 2 // CHUNKS
    rows = skeleton // CHUNKS
    count = boxes * neighbours * (neighbours + 1) // 2
    bf16, f32 = jnp.bfloat16, jnp.float32
    anywhere = pl.BlockSpec(memory_space=pl.ANY)
    on_chip = pl.BlockSpec(memory_space=pltpu.VMEM)
    dma = pltpu.SemaphoreType.DMA
    updated, panel = pl.pallas_call(
        functools.partial(kernel, n_surf, n_pair),
        name="eliminate",
        out_shape=(
            pltpu.VMEM(blocks.shape, f32),
            pltpu.VMEM((skeleton, columns), f32),
        ),
        in_specs=[anywhere] * 6,
        out_specs=(on_chip, on_chip),
        scratch_shapes=[
            pltpu.SMEM((boxes, neighbours, neighbours), jnp.int32),
            pltpu.VMEM((boxes, neighbours, skeleton, redundant), bf16),
            pltpu.VMEM((boxes, neighbours, skeleton, redundant), bf16),
            pltpu.VMEM(inverse.shape, bf16),
            pltpu.VMEM(blocks.shape, f32),
            pltpu.VMEM((boxes, neighbours, skeleton, 2 * redundant), bf16),
            pltpu.VMEM((boxes, neighbours, 2 * redundant, 256), bf16),
            pltpu.VMEM((count + 1, CHUNKS * packed, 128), f32),
            pltpu.SMEM((count + SPOTS * local,), jnp.int32),
            pltpu.VMEM((4, CHUNKS, local, packed, 128), bf16),
            pltpu.VMEM((4, CHUNKS, local, packed, 128), bf16),
            pltpu.VMEM((local, skeleton, columns), bf16),
            pltpu.VMEM(((n_pair - 1) * local, skeleton, columns), bf16),
            pltpu.VMEM((local, rows, skeleton), bf16),
            pltpu.VMEM((n_pair - 1, CHUNKS, rows, columns), bf16),
            pltpu.VMEM((n_pair - 1, CHUNKS, rows, columns), bf16),
            dma((6,)),
            dma,
            dma,
            dma((4, CHUNKS)),
            dma,
            dma,
            dma,
            dma,
        ],
        compiler_params=pltpu.CompilerParams(collective_id=0, has_side_effects=True, vmem_limit_bytes=VMEM),
    )(target, jnp.swapaxes(left, 2, 3), jnp.swapaxes(right, 2, 3), inverse, blocks, weights)
    return pl.pallas_call(
        store,
        name="store",
        out_shape=(
            jax.ShapeDtypeStruct(blocks.shape, f32),
            jax.ShapeDtypeStruct((skeleton, columns), f32),
        ),
        in_specs=[anywhere] * 2,
        out_specs=(anywhere, anywhere),
        scratch_shapes=[dma((2,))],
        compiler_params=pltpu.CompilerParams(vmem_limit_bytes=2**20),
    )(updated, panel)


def solution(mesh):
    in_specs = (
        P(("surf", "pair"), None, None, None),
        P(("surf", "pair"), None, None, None),
        P(("surf", "pair"), None, None),
        P(("surf", "pair"), None, None),
        P(("surf", "pair"), None, None),
        P("surf", None, "pair"),
    )
    out_specs = (P(("surf", "pair"), None, None), P("surf", "pair"))
    return jax.shard_map(body, mesh=mesh, in_specs=in_specs, out_specs=out_specs, check_vma=False)
```

```python
import functools

import jax
import jax.numpy as jnp
from jax import lax
from jax.experimental import pallas as pl
from jax.experimental.pallas import tpu as pltpu
from jax.sharding import PartitionSpec as P

MESH = pl.DeviceIdType.MESH
REACH = 2
SPOTS = 2 * REACH + 1
CHUNKS = 3
VMEM = 66048000
RELAY, PARTNER, NEAR, FAR = 0, 1, 2, 3
SPOT_OF = {RELAY: 0, PARTNER: 1, NEAR: 3, FAR: 4}
OWN_SPOT = 2


def kernel(
    n_surf, n_pair, target, left, right, inverse, blocks, weights, updated, coarse,
    target_s, left_v, right_v, inverse_v, blocks_v, rows_a, cols_b, acc, index, pieces, arrived,
    weights_own, weights_in, rounded, part, part_in,
    load_sem, send_sem, partner_sem, recv_sem, wsend_sem, wrecv_sem, psend_sem, precv_sem,
):
    boxes, neighbours, skeleton, redundant = left.shape
    local = blocks.shape[0]
    rows = skeleton // CHUNKS
    half = rows // 2
    packed = rows + half
    surf = lax.axis_index("surf")
    pair = lax.axis_index("pair")
    out = 2 * lax.rem(surf, 2) - 1

    def tile(offset):
        return lax.rem(surf + out * offset + n_surf, n_surf)

    def across(offset):
        return lax.rem(pair + offset, n_pair)

    loads = [
        pltpu.make_async_copy(source, into, load_sem.at[at])
        for at, (source, into) in enumerate(
            [
                (target, target_s),
                (inverse, inverse_v),
                (right, right_v),
                (left, left_v),
                (weights.at[pl.ds(pair * local, local)], weights_own),
                (blocks, blocks_v),
            ]
        )
    ]
    for load in loads:
        load.start()

    barrier = pltpu.get_barrier_semaphore()
    late = jnp.maximum(REACH - surf, 0)

    def greet(closing):
        for offset in range(-REACH, REACH + 1):
            if offset != 0:
                peer = surf + offset
                closes = jnp.logical_or(peer < 0, peer >= n_surf)

                @pl.when(closes if closing else jnp.logical_not(closes))
                def _():
                    there = lax.rem(peer + n_surf, n_surf)
                    pl.semaphore_signal(barrier, inc=1, device_id=(there, pair), device_id_type=MESH)

    for offset in range(1, n_pair):
        pl.semaphore_signal(barrier, inc=1, device_id=(surf, across(offset)), device_id_type=MESH)
    greet(False)

    for load in loads[:4]:
        load.wait()

    units = [(b, k, l) for b in range(boxes) for l in range(neighbours) for k in range(l + 1)]
    count = len(units)
    where_to = []
    for b, k, l in units:
        block = target_s[b, k, l]
        ahead = lax.rem(block // (local * n_pair) - surf + n_surf, n_surf)
        ahead = jnp.where(ahead <= REACH, ahead, ahead - n_surf)
        where_to.append((ahead * out + REACH) * local + lax.rem(block, local))
    for u in range(count):
        before = jnp.int32(count)
        for v in range(u):
            before = jnp.where(where_to[v] == where_to[u], v, before)
        index[u] = before
    for d in range(SPOTS * local):
        last = jnp.int32(count)
        for u in range(count):
            last = jnp.where(where_to[u] == d, u, last)
        index[count + d] = last

    acc[count] = jnp.zeros(acc.shape[1:], jnp.float32)

    for b in range(boxes):
        solved = lax.dot_general(
            right_v[b].reshape(neighbours * skeleton, redundant),
            inverse_v[b],
            (((1,), (1,)), ((), ())),
            preferred_element_type=jnp.float32,
        ).astype(jnp.bfloat16)
        for k in range(neighbours):
            mine = solved[k * skeleton : (k + 1) * skeleton]
            panel = left_v[b, k]
            for r in range(CHUNKS):
                rows_a[b, r, k, :, :redundant] = panel[r * rows : (r + 1) * rows]
                rows_a[b, r, k, :, redundant:] = mine[r * rows : (r + 1) * rows]
            both = jnp.concatenate([mine, panel], axis=1)
            both = jnp.concatenate([both, both[redundant:]], axis=0)
            cols_b[b, k] = both.T

    lanes = lax.broadcasted_iota(jnp.int32, (half, 128), 1)

    def make_units(r):
        top = r * packed
        for b in range(boxes):
            for l in range(neighbours):
                found = []
                if l > 0:
                    stacked = jnp.dot(
                        rows_a[b, r, :l].reshape(l * rows, 2 * redundant),
                        cols_b[b, l],
                        preferred_element_type=jnp.float32,
                    )
                    found = [stacked[k * rows : (k + 1) * rows] for k in range(l)]
                found.append(
                    jnp.dot(
                        rows_a[b, r, l, :, :redundant],
                        cols_b[b, l, :redundant],
                        preferred_element_type=jnp.float32,
                    )
                )
                for k, unit in enumerate(found):
                    u = units.index((b, k, l))
                    before = index[u]
                    acc[u, top : top + rows] = unit[:, :128] + acc[before, top : top + rows]
                    tail = jnp.where(lanes < 64, unit[:half, 128:], unit[half:, 128:])
                    acc[u, top + rows : top + packed] = tail + acc[before, top + rows : top + packed]

    make_units(0)
    pl.semaphore_wait(barrier, 2 * REACH + n_pair - 1 - late)
    greet(True)

    for offset in (2, 1, 3):
        slot = n_pair - offset
        copy = pltpu.make_async_remote_copy(
            src_ref=weights.at[pl.ds(across(offset) * local, local)],
            dst_ref=weights_in.at[pl.ds((slot - 1) * local, local)],
            send_sem=wsend_sem,
            recv_sem=wrecv_sem,
            device_id=(surf, across(offset)),
            device_id_type=MESH,
        )
        copy.start()

    def piece_of(spot, slot, r):
        return acc[index[count + spot * local + slot], r * packed : (r + 1) * packed]

    to = {RELAY: -1, PARTNER: -1, NEAR: 1, FAR: 2}

    def all_sent(source, into, sem):
        pltpu.make_async_remote_copy(
            src_ref=source, dst_ref=into, send_sem=sem, recv_sem=sem, device_id=(surf, across(1)), device_id_type=MESH
        ).wait_send()

    def all_in(source, into, sem):
        pltpu.make_async_remote_copy(
            src_ref=source, dst_ref=into, send_sem=sem, recv_sem=sem, device_id=(surf, across(1)), device_id_type=MESH
        ).wait_recv()

    def to_send(kind, r):
        return pltpu.make_async_remote_copy(
            src_ref=pieces.at[kind, r],
            dst_ref=arrived.at[kind, r],
            send_sem=send_sem,
            recv_sem=partner_sem if kind == PARTNER else recv_sem.at[kind, r],
            device_id=(tile(to[kind]), pair),
            device_id_type=MESH,
        )

    copies = {}
    for r in range(CHUNKS):
        if r > 0:
            make_units(r)
        for kind in (RELAY, FAR, PARTNER):
            for slot in range(local):
                pieces[kind, r, slot] = piece_of(SPOT_OF[kind], slot, r).astype(jnp.bfloat16)
            copies[kind, r] = to_send(kind, r)
            if kind == FAR:
                pl.when(surf != 0)(copies[kind, r].start)
            else:
                copies[kind, r].start()

    @pl.when(surf == 0)
    def _():
        pl.semaphore_wait(barrier, REACH)
        for r in range(CHUNKS):
            copies[FAR, r].start()

    for r in range(CHUNKS):
        copies[RELAY, r].wait_recv()
        for slot in range(local):
            joined = piece_of(SPOT_OF[NEAR], slot, r) + arrived[RELAY, r, slot].astype(jnp.float32)
            pieces[NEAR, r, slot] = joined.astype(jnp.bfloat16)
        copies[NEAR, r] = to_send(NEAR, r)
        copies[NEAR, r].start()

    loads[4].wait()
    loads[5].wait()
    own = []
    for r in range(CHUNKS):
        top = r * rows
        if r == 0:
            all_in(pieces.at[PARTNER], arrived.at[PARTNER], partner_sem)
        for kind in (FAR, NEAR):
            copies[kind, r].wait_recv()
        for slot in range(local):
            total = piece_of(OWN_SPOT, slot, r)
            for kind in (PARTNER, FAR, NEAR):
                total = total + arrived[kind, r, slot].astype(jnp.float32)
            tail = total[rows:]
            tail = jnp.concatenate([tail, pltpu.roll(tail, 64, axis=1)], axis=0)[:, :64]
            main = blocks_v[slot, top : top + rows, :128] - total[:rows]
            tail = blocks_v[slot, top : top + rows, 128:] - tail
            updated[slot, top : top + rows, :128] = main
            updated[slot, top : top + rows, 128:] = tail
            rounded[slot, :, :128] = main.astype(jnp.bfloat16)
            rounded[slot, :, 128:] = tail.astype(jnp.bfloat16)
        if r == 0:
            all_in(weights.at[pl.ds(0, (n_pair - 1) * local)], weights_in, wrecv_sem)

        def weights_of(offset, slot):
            return weights_own[slot] if offset == 0 else weights_in[(offset - 1) * local + slot]

        def panel_of(first, second):
            total = None
            for slot in range(local):
                both = jnp.concatenate([weights_of(first, slot), weights_of(second, slot)], axis=1)
                term = jnp.dot(rounded[slot], both, preferred_element_type=jnp.float32)
                total = term if total is None else total + term
            return total

        def send_part(offset, value):
            part[offset - 1, r] = value.astype(jnp.bfloat16)
            slot = n_pair - offset - 1
            copy = pltpu.make_async_remote_copy(
                src_ref=part.at[offset - 1, r],
                dst_ref=part_in.at[slot, r],
                send_sem=psend_sem,
                recv_sem=precv_sem,
                device_id=(surf, across(offset)),
                device_id_type=MESH,
            )
            copy.start()

        panel = panel_of(2, 1)
        send_part(2, panel[:, :128])
        send_part(1, panel[:, 128:])
        panel = panel_of(3, 0)
        send_part(3, panel[:, :128])
        coarse[top : top + rows] = panel[:, 128:]

    all_in(part, part_in, precv_sem)
    for r in range(CHUNKS):
        top = r * rows
        total = coarse[top : top + rows]
        for slot in range(n_pair - 1):
            total = total + part_in[slot, r].astype(jnp.float32)
        coarse[top : top + rows] = total

    @pl.when(surf == 1)
    def _():
        pl.semaphore_wait(barrier, 1)

    all_sent(weights.at[pl.ds(0, (n_pair - 1) * local)], weights_in, wsend_sem)
    all_sent(pieces, arrived, send_sem)
    all_sent(part, part_in, psend_sem)


def store(updated, coarse, updated_out, coarse_out, sem):
    copies = [
        pltpu.make_async_copy(updated, updated_out, sem.at[0]),
        pltpu.make_async_copy(coarse, coarse_out, sem.at[1]),
    ]
    for copy in copies:
        copy.start()
    for copy in copies:
        copy.wait()


def body(left, right, inverse, target, blocks, weights):
    n_surf = lax.axis_size("surf")
    n_pair = lax.axis_size("pair")
    boxes, neighbours, redundant, skeleton = left.shape
    local = blocks.shape[0]
    columns = weights.shape[2]
    packed = skeleton * 3 // 2 // CHUNKS
    rows = skeleton // CHUNKS
    count = boxes * neighbours * (neighbours + 1) // 2
    bf16, f32 = jnp.bfloat16, jnp.float32
    anywhere = pl.BlockSpec(memory_space=pl.ANY)
    on_chip = pl.BlockSpec(memory_space=pltpu.VMEM)
    dma = pltpu.SemaphoreType.DMA
    updated, panel = pl.pallas_call(
        functools.partial(kernel, n_surf, n_pair),
        name="eliminate",
        out_shape=(
            pltpu.VMEM(blocks.shape, f32),
            pltpu.VMEM((skeleton, columns), f32),
        ),
        in_specs=[anywhere] * 6,
        out_specs=(on_chip, on_chip),
        scratch_shapes=[
            pltpu.SMEM((boxes, neighbours, neighbours), jnp.int32),
            pltpu.VMEM((boxes, neighbours, skeleton, redundant), bf16),
            pltpu.VMEM((boxes, neighbours, skeleton, redundant), bf16),
            pltpu.VMEM(inverse.shape, bf16),
            pltpu.VMEM(blocks.shape, f32),
            pltpu.VMEM((boxes, CHUNKS, neighbours, rows, 2 * redundant), bf16),
            pltpu.VMEM((boxes, neighbours, 2 * redundant, 256), bf16),
            pltpu.VMEM((count + 1, CHUNKS * packed, 128), f32),
            pltpu.SMEM((count + SPOTS * local,), jnp.int32),
            pltpu.VMEM((4, CHUNKS, local, packed, 128), bf16),
            pltpu.VMEM((4, CHUNKS, local, packed, 128), bf16),
            pltpu.VMEM((local, skeleton, columns), bf16),
            pltpu.VMEM(((n_pair - 1) * local, skeleton, columns), bf16),
            pltpu.VMEM((local, rows, skeleton), bf16),
            pltpu.VMEM((n_pair - 1, CHUNKS, rows, columns), bf16),
            pltpu.VMEM((n_pair - 1, CHUNKS, rows, columns), bf16),
            dma((6,)),
            dma,
            dma,
            dma((4, CHUNKS)),
            dma,
            dma,
            dma,
            dma,
        ],
        compiler_params=pltpu.CompilerParams(collective_id=0, has_side_effects=True, vmem_limit_bytes=VMEM),
    )(target, jnp.swapaxes(left, 2, 3), jnp.swapaxes(right, 2, 3), inverse, blocks, weights)
    return pl.pallas_call(
        store,
        name="store",
        out_shape=(
            jax.ShapeDtypeStruct(blocks.shape, f32),
            jax.ShapeDtypeStruct((skeleton, columns), f32),
        ),
        in_specs=[anywhere] * 2,
        out_specs=(anywhere, anywhere),
        scratch_shapes=[dma((2,))],
        compiler_params=pltpu.CompilerParams(vmem_limit_bytes=2**20),
    )(updated, panel)


def solution(mesh):
    in_specs = (
        P(("surf", "pair"), None, None, None),
        P(("surf", "pair"), None, None, None),
        P(("surf", "pair"), None, None),
        P(("surf", "pair"), None, None),
        P(("surf", "pair"), None, None),
        P("surf", None, "pair"),
    )
    out_specs = (P(("surf", "pair"), None, None), P("surf", "pair"))
    return jax.shard_map(body, mesh=mesh, in_specs=in_specs, out_specs=out_specs, check_vma=False)
```

```python
import functools

import jax
import jax.numpy as jnp
from jax import lax
from jax.experimental import pallas as pl
from jax.experimental.pallas import tpu as pltpu
from jax.sharding import PartitionSpec as P

MESH = pl.DeviceIdType.MESH
REACH = 2
SPOTS = 2 * REACH + 1
CHUNKS = 3
VMEM = 66048000
RELAY, PARTNER, NEAR, FAR = 0, 1, 2, 3
SPOT_OF = {RELAY: 0, PARTNER: 1, NEAR: 3, FAR: 4}
OWN_SPOT = 2


def kernel(
    n_surf, n_pair, target, left, right, inverse, blocks, weights, updated, coarse,
    target_s, left_v, right_v, inverse_v, blocks_v, rows_a, cols_b, acc, index, pieces, arrived,
    weights_own, weights_in, rounded, part, part_in,
    load_sem, send_sem, relay_sem, recv_sem, wsend_sem, wrecv_sem, psend_sem, precv_sem,
):
    boxes, neighbours, skeleton, redundant = left.shape
    local = blocks.shape[0]
    rows = skeleton // CHUNKS
    half = rows // 2
    packed = rows + half
    surf = lax.axis_index("surf")
    pair = lax.axis_index("pair")
    out = 2 * lax.rem(surf, 2) - 1

    def tile(offset):
        return lax.rem(surf + out * offset + n_surf, n_surf)

    def across(offset):
        return lax.rem(pair + offset, n_pair)

    loads = [
        pltpu.make_async_copy(source, into, load_sem.at[at])
        for at, (source, into) in enumerate(
            [
                (target, target_s),
                (inverse, inverse_v),
                (right, right_v),
                (left, left_v),
                (weights.at[pl.ds(pair * local, local)], weights_own),
                (blocks, blocks_v),
            ]
        )
    ]
    for load in loads:
        load.start()

    barrier = pltpu.get_barrier_semaphore()
    late = jnp.maximum(REACH - surf, 0)

    def greet(closing):
        for offset in range(-REACH, REACH + 1):
            if offset != 0:
                peer = surf + offset
                closes = jnp.logical_or(peer < 0, peer >= n_surf)

                @pl.when(closes if closing else jnp.logical_not(closes))
                def _():
                    there = lax.rem(peer + n_surf, n_surf)
                    pl.semaphore_signal(barrier, inc=1, device_id=(there, pair), device_id_type=MESH)

    for offset in range(1, n_pair):
        pl.semaphore_signal(barrier, inc=1, device_id=(surf, across(offset)), device_id_type=MESH)
    greet(False)

    for load in loads[:4]:
        load.wait()

    units = [(b, k, l) for b in range(boxes) for l in range(neighbours) for k in range(l + 1)]
    count = len(units)
    where_to = []
    for b, k, l in units:
        block = target_s[b, k, l]
        ahead = lax.rem(block // (local * n_pair) - surf + n_surf, n_surf)
        ahead = jnp.where(ahead <= REACH, ahead, ahead - n_surf)
        where_to.append((ahead * out + REACH) * local + lax.rem(block, local))
    for u in range(count):
        before = jnp.int32(count)
        for v in range(u):
            before = jnp.where(where_to[v] == where_to[u], v, before)
        index[u] = before
    for d in range(SPOTS * local):
        last = jnp.int32(count)
        for u in range(count):
            last = jnp.where(where_to[u] == d, u, last)
        index[count + d] = last

    acc[count] = jnp.zeros(acc.shape[1:], jnp.float32)

    for b in range(boxes):
        solved = lax.dot_general(
            right_v[b].reshape(neighbours * skeleton, redundant),
            inverse_v[b],
            (((1,), (1,)), ((), ())),
            preferred_element_type=jnp.float32,
        ).astype(jnp.bfloat16)
        for k in range(neighbours):
            mine = solved[k * skeleton : (k + 1) * skeleton]
            panel = left_v[b, k]
            for r in range(CHUNKS):
                rows_a[b, r, k, :, :redundant] = panel[r * rows : (r + 1) * rows]
                rows_a[b, r, k, :, redundant:] = mine[r * rows : (r + 1) * rows]
            both = jnp.concatenate([mine, panel], axis=1)
            both = jnp.concatenate([both, both[redundant:]], axis=0)
            cols_b[b, k] = both.T

    lanes = lax.broadcasted_iota(jnp.int32, (half, 128), 1)

    def make_units(r):
        top = r * packed
        for b in range(boxes):
            for l in range(neighbours):
                found = []
                if l > 0:
                    stacked = jnp.dot(
                        rows_a[b, r, :l].reshape(l * rows, 2 * redundant),
                        cols_b[b, l],
                        preferred_element_type=jnp.float32,
                    )
                    found = [stacked[k * rows : (k + 1) * rows] for k in range(l)]
                found.append(
                    jnp.dot(
                        rows_a[b, r, l, :, :redundant],
                        cols_b[b, l, :redundant],
                        preferred_element_type=jnp.float32,
                    )
                )
                for k, unit in enumerate(found):
                    u = units.index((b, k, l))
                    before = index[u]
                    acc[u, top : top + rows] = unit[:, :128] + acc[before, top : top + rows]
                    tail = jnp.where(lanes < 64, unit[:half, 128:], unit[half:, 128:])
                    acc[u, top + rows : top + packed] = tail + acc[before, top + rows : top + packed]

    make_units(0)
    pl.semaphore_wait(barrier, 2 * REACH + n_pair - 1 - late)
    greet(True)

    for offset in (2, 1, 3):
        slot = n_pair - offset
        copy = pltpu.make_async_remote_copy(
            src_ref=weights.at[pl.ds(across(offset) * local, local)],
            dst_ref=weights_in.at[pl.ds((slot - 1) * local, local)],
            send_sem=wsend_sem,
            recv_sem=wrecv_sem,
            device_id=(surf, across(offset)),
            device_id_type=MESH,
        )
        copy.start()

    def piece_of(spot, slot, r):
        return acc[index[count + spot * local + slot], r * packed : (r + 1) * packed]

    to = {RELAY: -1, PARTNER: -1, NEAR: 1, FAR: 2}

    def all_sent(source, into, sem):
        pltpu.make_async_remote_copy(
            src_ref=source, dst_ref=into, send_sem=sem, recv_sem=sem, device_id=(surf, across(1)), device_id_type=MESH
        ).wait_send()

    def all_in(source, into, sem):
        pltpu.make_async_remote_copy(
            src_ref=source, dst_ref=into, send_sem=sem, recv_sem=sem, device_id=(surf, across(1)), device_id_type=MESH
        ).wait_recv()

    def to_send(kind, r):
        return pltpu.make_async_remote_copy(
            src_ref=pieces.at[kind, r],
            dst_ref=arrived.at[kind, r],
            send_sem=send_sem,
            recv_sem=relay_sem.at[r] if kind == RELAY else recv_sem.at[r],
            device_id=(tile(to[kind]), pair),
            device_id_type=MESH,
        )

    copies = {}
    for r in range(CHUNKS):
        if r > 0:
            make_units(r)
        for kind in (RELAY, FAR, PARTNER):
            for slot in range(local):
                pieces[kind, r, slot] = piece_of(SPOT_OF[kind], slot, r).astype(jnp.bfloat16)
            copies[kind, r] = to_send(kind, r)
            if kind == FAR:
                pl.when(surf != 0)(copies[kind, r].start)
            else:
                copies[kind, r].start()

    @pl.when(surf == 0)
    def _():
        pl.semaphore_wait(barrier, REACH)
        for r in range(CHUNKS):
            copies[FAR, r].start()

    for r in range(CHUNKS):
        copies[RELAY, r].wait_recv()
        for slot in range(local):
            joined = piece_of(SPOT_OF[NEAR], slot, r) + arrived[RELAY, r, slot].astype(jnp.float32)
            pieces[NEAR, r, slot] = joined.astype(jnp.bfloat16)
        copies[NEAR, r] = to_send(NEAR, r)
        copies[NEAR, r].start()

    loads[4].wait()
    loads[5].wait()
    own = []
    for r in range(CHUNKS):
        top = r * rows
        others = pl.ds(PARTNER, 3)
        all_in(pieces.at[others, r], arrived.at[others, r], recv_sem.at[r])
        for slot in range(local):
            total = piece_of(OWN_SPOT, slot, r)
            for kind in (PARTNER, FAR, NEAR):
                total = total + arrived[kind, r, slot].astype(jnp.float32)
            tail = total[rows:]
            tail = jnp.concatenate([tail, pltpu.roll(tail, 64, axis=1)], axis=0)[:, :64]
            main = blocks_v[slot, top : top + rows, :128] - total[:rows]
            tail = blocks_v[slot, top : top + rows, 128:] - tail
            updated[slot, top : top + rows, :128] = main
            updated[slot, top : top + rows, 128:] = tail
            rounded[slot, :, :128] = main.astype(jnp.bfloat16)
            rounded[slot, :, 128:] = tail.astype(jnp.bfloat16)
        if r == 0:
            all_in(weights.at[pl.ds(0, (n_pair - 1) * local)], weights_in, wrecv_sem)

        def weights_of(offset, slot):
            return weights_own[slot] if offset == 0 else weights_in[(offset - 1) * local + slot]

        def panel_of(*offsets):
            total = None
            for slot in range(local):
                factor = [weights_of(offset, slot) for offset in offsets]
                factor = jnp.concatenate(factor, axis=1) if len(factor) > 1 else factor[0]
                term = jnp.dot(rounded[slot], factor, preferred_element_type=jnp.float32)
                total = term if total is None else total + term
            return total

        def send_part(offset, value):
            part[offset - 1, r] = value.astype(jnp.bfloat16)
            slot = n_pair - offset - 1
            copy = pltpu.make_async_remote_copy(
                src_ref=part.at[offset - 1, r],
                dst_ref=part_in.at[slot, r],
                send_sem=psend_sem,
                recv_sem=precv_sem,
                device_id=(surf, across(offset)),
                device_id_type=MESH,
            )
            copy.start()

        send_part(2, panel_of(2))
        panel = panel_of(1, 3)
        send_part(1, panel[:, :128])
        send_part(3, panel[:, 128:])
        coarse[top : top + rows] = panel_of(0)

    all_in(part, part_in, precv_sem)
    for r in range(CHUNKS):
        top = r * rows
        total = coarse[top : top + rows]
        for slot in range(n_pair - 1):
            total = total + part_in[slot, r].astype(jnp.float32)
        coarse[top : top + rows] = total

    @pl.when(surf == 1)
    def _():
        pl.semaphore_wait(barrier, 1)

    all_sent(weights.at[pl.ds(0, (n_pair - 1) * local)], weights_in, wsend_sem)
    all_sent(pieces, arrived, send_sem)
    all_sent(part, part_in, psend_sem)


def store(updated, coarse, updated_out, coarse_out, sem):
    copies = [
        pltpu.make_async_copy(updated, updated_out, sem.at[0]),
        pltpu.make_async_copy(coarse, coarse_out, sem.at[1]),
    ]
    for copy in copies:
        copy.start()
    for copy in copies:
        copy.wait()


def body(left, right, inverse, target, blocks, weights):
    n_surf = lax.axis_size("surf")
    n_pair = lax.axis_size("pair")
    boxes, neighbours, redundant, skeleton = left.shape
    local = blocks.shape[0]
    columns = weights.shape[2]
    packed = skeleton * 3 // 2 // CHUNKS
    rows = skeleton // CHUNKS
    count = boxes * neighbours * (neighbours + 1) // 2
    bf16, f32 = jnp.bfloat16, jnp.float32
    anywhere = pl.BlockSpec(memory_space=pl.ANY)
    on_chip = pl.BlockSpec(memory_space=pltpu.VMEM)
    dma = pltpu.SemaphoreType.DMA
    updated, panel = pl.pallas_call(
        functools.partial(kernel, n_surf, n_pair),
        name="eliminate",
        out_shape=(
            pltpu.VMEM(blocks.shape, f32),
            pltpu.VMEM((skeleton, columns), f32),
        ),
        in_specs=[anywhere] * 6,
        out_specs=(on_chip, on_chip),
        scratch_shapes=[
            pltpu.SMEM((boxes, neighbours, neighbours), jnp.int32),
            pltpu.VMEM((boxes, neighbours, skeleton, redundant), bf16),
            pltpu.VMEM((boxes, neighbours, skeleton, redundant), bf16),
            pltpu.VMEM(inverse.shape, bf16),
            pltpu.VMEM(blocks.shape, f32),
            pltpu.VMEM((boxes, CHUNKS, neighbours, rows, 2 * redundant), bf16),
            pltpu.VMEM((boxes, neighbours, 2 * redundant, 256), bf16),
            pltpu.VMEM((count + 1, CHUNKS * packed, 128), f32),
            pltpu.SMEM((count + SPOTS * local,), jnp.int32),
            pltpu.VMEM((4, CHUNKS, local, packed, 128), bf16),
            pltpu.VMEM((4, CHUNKS, local, packed, 128), bf16),
            pltpu.VMEM((local, skeleton, columns), bf16),
            pltpu.VMEM(((n_pair - 1) * local, skeleton, columns), bf16),
            pltpu.VMEM((local, rows, skeleton), bf16),
            pltpu.VMEM((n_pair - 1, CHUNKS, rows, columns), bf16),
            pltpu.VMEM((n_pair - 1, CHUNKS, rows, columns), bf16),
            dma((6,)),
            dma,
            dma((CHUNKS,)),
            dma((CHUNKS,)),
            dma,
            dma,
            dma,
            dma,
        ],
        compiler_params=pltpu.CompilerParams(collective_id=0, has_side_effects=True, vmem_limit_bytes=VMEM),
    )(target, jnp.swapaxes(left, 2, 3), jnp.swapaxes(right, 2, 3), inverse, blocks, weights)
    return pl.pallas_call(
        store,
        name="store",
        out_shape=(
            jax.ShapeDtypeStruct(blocks.shape, f32),
            jax.ShapeDtypeStruct((skeleton, columns), f32),
        ),
        in_specs=[anywhere] * 2,
        out_specs=(anywhere, anywhere),
        scratch_shapes=[dma((2,))],
        compiler_params=pltpu.CompilerParams(vmem_limit_bytes=2**20),
    )(updated, panel)


def solution(mesh):
    in_specs = (
        P(("surf", "pair"), None, None, None),
        P(("surf", "pair"), None, None, None),
        P(("surf", "pair"), None, None),
        P(("surf", "pair"), None, None),
        P(("surf", "pair"), None, None),
        P("surf", None, "pair"),
    )
    out_specs = (P(("surf", "pair"), None, None), P("surf", "pair"))
    return jax.shard_map(body, mesh=mesh, in_specs=in_specs, out_specs=out_specs, check_vma=False)
```

```python
import functools

import jax
import jax.numpy as jnp
from jax import lax
from jax.experimental import pallas as pl
from jax.experimental.pallas import tpu as pltpu
from jax.sharding import PartitionSpec as P

MESH = pl.DeviceIdType.MESH
REACH = 2
SPOTS = 2 * REACH + 1
CHUNKS = 3
VMEM = 66048000
RELAY, PARTNER, NEAR, FAR = 0, 1, 2, 3
SPOT_OF = {RELAY: 0, PARTNER: 1, NEAR: 3, FAR: 4}
OWN_SPOT = 2


def kernel(
    n_surf, n_pair, target, left, right, inverse, blocks, weights, updated, coarse,
    target_s, left_v, right_v, inverse_v, blocks_v, rows_a, cols_b, acc, index, pieces, arrived,
    weights_own, weights_in, rounded, part, part_in,
    load_sem, send_sem, relay_sem, recv_sem, wsend_sem, wrecv_sem, psend_sem, precv_sem,
):
    boxes, neighbours, skeleton, redundant = left.shape
    local = blocks.shape[0]
    rows = skeleton // CHUNKS
    half = rows // 2
    packed = rows + half
    surf = lax.axis_index("surf")
    pair = lax.axis_index("pair")
    out = 2 * lax.rem(surf, 2) - 1

    def tile(offset):
        return lax.rem(surf + out * offset + n_surf, n_surf)

    def across(offset):
        return lax.rem(pair + offset, n_pair)

    loads = [
        pltpu.make_async_copy(source, into, load_sem.at[at])
        for at, (source, into) in enumerate(
            [
                (target, target_s),
                (inverse, inverse_v),
                (right, right_v),
                (left, left_v),
                (weights.at[pl.ds(pair * local, local)], weights_own),
                (blocks, blocks_v),
            ]
        )
    ]
    for load in loads:
        load.start()

    barrier = pltpu.get_barrier_semaphore()
    late = jnp.maximum(REACH - surf, 0)

    def greet(closing):
        for offset in range(-REACH, REACH + 1):
            if offset != 0:
                peer = surf + offset
                closes = jnp.logical_or(peer < 0, peer >= n_surf)

                @pl.when(closes if closing else jnp.logical_not(closes))
                def _():
                    there = lax.rem(peer + n_surf, n_surf)
                    pl.semaphore_signal(barrier, inc=1, device_id=(there, pair), device_id_type=MESH)

    for offset in range(1, n_pair):
        pl.semaphore_signal(barrier, inc=1, device_id=(surf, across(offset)), device_id_type=MESH)
    greet(False)

    for load in loads[:4]:
        load.wait()

    units = [(b, k, l) for b in range(boxes) for l in range(neighbours) for k in range(l + 1)]
    count = len(units)
    where_to = []
    for b, k, l in units:
        block = target_s[b, k, l]
        ahead = lax.rem(block // (local * n_pair) - surf + n_surf, n_surf)
        ahead = jnp.where(ahead <= REACH, ahead, ahead - n_surf)
        where_to.append((ahead * out + REACH) * local + lax.rem(block, local))
    for u in range(count):
        before = jnp.int32(count)
        for v in range(u):
            before = jnp.where(where_to[v] == where_to[u], v, before)
        index[u] = before
    for d in range(SPOTS * local):
        last = jnp.int32(count)
        for u in range(count):
            last = jnp.where(where_to[u] == d, u, last)
        index[count + d] = last

    acc[count] = jnp.zeros(acc.shape[1:], jnp.float32)

    for b in range(boxes):
        solved = lax.dot_general(
            right_v[b].reshape(neighbours * skeleton, redundant),
            inverse_v[b],
            (((1,), (1,)), ((), ())),
            preferred_element_type=jnp.float32,
        ).astype(jnp.bfloat16)
        for k in range(neighbours):
            mine = solved[k * skeleton : (k + 1) * skeleton]
            panel = left_v[b, k]
            for r in range(CHUNKS):
                rows_a[b, r, k, :, :redundant] = panel[r * rows : (r + 1) * rows]
                rows_a[b, r, k, :, redundant:] = mine[r * rows : (r + 1) * rows]
            cols_b[b, k, :redundant] = jnp.concatenate([mine, mine[128:]], axis=0).T
            cols_b[b, k, redundant:] = jnp.concatenate([panel, panel[128:]], axis=0).T

    lanes = lax.broadcasted_iota(jnp.int32, (half, 128), 1)

    def make_units(r):
        top = r * packed
        for b in range(boxes):
            for l in range(neighbours):
                found = []
                if l > 0:
                    stacked = jnp.dot(
                        rows_a[b, r, :l].reshape(l * rows, 2 * redundant),
                        cols_b[b, l],
                        preferred_element_type=jnp.float32,
                    )
                    found = [stacked[k * rows : (k + 1) * rows] for k in range(l)]
                found.append(
                    jnp.dot(
                        rows_a[b, r, l, :, :redundant],
                        cols_b[b, l, :redundant],
                        preferred_element_type=jnp.float32,
                    )
                )
                for k, unit in enumerate(found):
                    u = units.index((b, k, l))
                    before = index[u]
                    acc[u, top : top + rows] = unit[:, :128] + acc[before, top : top + rows]
                    tail = jnp.where(lanes < 64, unit[:half, 128:], unit[half:, 128:])
                    acc[u, top + rows : top + packed] = tail + acc[before, top + rows : top + packed]

    make_units(0)
    pl.semaphore_wait(barrier, 2 * REACH + n_pair - 1 - late)
    greet(True)

    for offset in (2, 1, 3):
        slot = n_pair - offset
        copy = pltpu.make_async_remote_copy(
            src_ref=weights.at[pl.ds(across(offset) * local, local)],
            dst_ref=weights_in.at[pl.ds((slot - 1) * local, local)],
            send_sem=wsend_sem,
            recv_sem=wrecv_sem,
            device_id=(surf, across(offset)),
            device_id_type=MESH,
        )
        copy.start()

    def piece_of(spot, slot, r):
        return acc[index[count + spot * local + slot], r * packed : (r + 1) * packed]

    to = {RELAY: -1, PARTNER: -1, NEAR: 1, FAR: 2}

    def all_sent(source, into, sem):
        pltpu.make_async_remote_copy(
            src_ref=source, dst_ref=into, send_sem=sem, recv_sem=sem, device_id=(surf, across(1)), device_id_type=MESH
        ).wait_send()

    def all_in(source, into, sem):
        pltpu.make_async_remote_copy(
            src_ref=source, dst_ref=into, send_sem=sem, recv_sem=sem, device_id=(surf, across(1)), device_id_type=MESH
        ).wait_recv()

    def to_send(kind, r):
        return pltpu.make_async_remote_copy(
            src_ref=pieces.at[kind, r],
            dst_ref=arrived.at[kind, r],
            send_sem=send_sem,
            recv_sem=relay_sem.at[r] if kind == RELAY else recv_sem.at[r],
            device_id=(tile(to[kind]), pair),
            device_id_type=MESH,
        )

    copies = {}
    for r in range(CHUNKS):
        if r > 0:
            make_units(r)
        for kind in (RELAY, FAR, PARTNER):
            for slot in range(local):
                pieces[kind, r, slot] = piece_of(SPOT_OF[kind], slot, r).astype(jnp.bfloat16)
            copies[kind, r] = to_send(kind, r)
            if kind == FAR:
                pl.when(surf != 0)(copies[kind, r].start)
            else:
                copies[kind, r].start()

    @pl.when(surf == 0)
    def _():
        pl.semaphore_wait(barrier, REACH)
        for r in range(CHUNKS):
            copies[FAR, r].start()

    for r in range(CHUNKS):
        copies[RELAY, r].wait_recv()
        for slot in range(local):
            joined = piece_of(SPOT_OF[NEAR], slot, r) + arrived[RELAY, r, slot].astype(jnp.float32)
            pieces[NEAR, r, slot] = joined.astype(jnp.bfloat16)
        copies[NEAR, r] = to_send(NEAR, r)
        copies[NEAR, r].start()

    loads[4].wait()
    loads[5].wait()
    own = []
    for r in range(CHUNKS):
        top = r * rows
        others = pl.ds(PARTNER, 3)
        all_in(pieces.at[others, r], arrived.at[others, r], recv_sem.at[r])
        for slot in range(local):
            total = piece_of(OWN_SPOT, slot, r)
            for kind in (PARTNER, FAR, NEAR):
                total = total + arrived[kind, r, slot].astype(jnp.float32)
            tail = total[rows:]
            tail = jnp.concatenate([tail, pltpu.roll(tail, 64, axis=1)], axis=0)[:, :64]
            main = blocks_v[slot, top : top + rows, :128] - total[:rows]
            tail = blocks_v[slot, top : top + rows, 128:] - tail
            updated[slot, top : top + rows, :128] = main
            updated[slot, top : top + rows, 128:] = tail
            rounded[slot, :, :128] = main.astype(jnp.bfloat16)
            rounded[slot, :, 128:] = tail.astype(jnp.bfloat16)
        if r == 0:
            all_in(weights.at[pl.ds(0, (n_pair - 1) * local)], weights_in, wrecv_sem)

        def weights_of(offset, slot):
            return weights_own[slot] if offset == 0 else weights_in[(offset - 1) * local + slot]

        def panel_of(*offsets):
            total = None
            for slot in range(local):
                factor = [weights_of(offset, slot) for offset in offsets]
                factor = jnp.concatenate(factor, axis=1) if len(factor) > 1 else factor[0]
                term = jnp.dot(rounded[slot], factor, preferred_element_type=jnp.float32)
                total = term if total is None else total + term
            return total

        def send_part(offset, value):
            part[offset - 1, r] = value.astype(jnp.bfloat16)
            slot = n_pair - offset - 1
            copy = pltpu.make_async_remote_copy(
                src_ref=part.at[offset - 1, r],
                dst_ref=part_in.at[slot, r],
                send_sem=psend_sem,
                recv_sem=precv_sem,
                device_id=(surf, across(offset)),
                device_id_type=MESH,
            )
            copy.start()

        send_part(2, panel_of(2))
        panel = panel_of(1, 3)
        send_part(1, panel[:, :128])
        send_part(3, panel[:, 128:])
        coarse[top : top + rows] = panel_of(0)

    all_in(part, part_in, precv_sem)
    for r in range(CHUNKS):
        top = r * rows
        total = coarse[top : top + rows]
        for slot in range(n_pair - 1):
            total = total + part_in[slot, r].astype(jnp.float32)
        coarse[top : top + rows] = total

    @pl.when(surf == 1)
    def _():
        pl.semaphore_wait(barrier, 1)

    all_sent(weights.at[pl.ds(0, (n_pair - 1) * local)], weights_in, wsend_sem)
    all_sent(pieces, arrived, send_sem)
    all_sent(part, part_in, psend_sem)


def store(updated, coarse, updated_out, coarse_out, sem):
    copies = [
        pltpu.make_async_copy(updated, updated_out, sem.at[0]),
        pltpu.make_async_copy(coarse, coarse_out, sem.at[1]),
    ]
    for copy in copies:
        copy.start()
    for copy in copies:
        copy.wait()


def body(left, right, inverse, target, blocks, weights):
    n_surf = lax.axis_size("surf")
    n_pair = lax.axis_size("pair")
    boxes, neighbours, redundant, skeleton = left.shape
    local = blocks.shape[0]
    columns = weights.shape[2]
    packed = skeleton * 3 // 2 // CHUNKS
    rows = skeleton // CHUNKS
    count = boxes * neighbours * (neighbours + 1) // 2
    bf16, f32 = jnp.bfloat16, jnp.float32
    anywhere = pl.BlockSpec(memory_space=pl.ANY)
    on_chip = pl.BlockSpec(memory_space=pltpu.VMEM)
    dma = pltpu.SemaphoreType.DMA
    updated, panel = pl.pallas_call(
        functools.partial(kernel, n_surf, n_pair),
        name="eliminate",
        out_shape=(
            pltpu.VMEM(blocks.shape, f32),
            pltpu.VMEM((skeleton, columns), f32),
        ),
        in_specs=[anywhere] * 6,
        out_specs=(on_chip, on_chip),
        scratch_shapes=[
            pltpu.SMEM((boxes, neighbours, neighbours), jnp.int32),
            pltpu.VMEM((boxes, neighbours, skeleton, redundant), bf16),
            pltpu.VMEM((boxes, neighbours, skeleton, redundant), bf16),
            pltpu.VMEM(inverse.shape, bf16),
            pltpu.VMEM(blocks.shape, f32),
            pltpu.VMEM((boxes, CHUNKS, neighbours, rows, 2 * redundant), bf16),
            pltpu.VMEM((boxes, neighbours, 2 * redundant, 256), bf16),
            pltpu.VMEM((count + 1, CHUNKS * packed, 128), f32),
            pltpu.SMEM((count + SPOTS * local,), jnp.int32),
            pltpu.VMEM((4, CHUNKS, local, packed, 128), bf16),
            pltpu.VMEM((4, CHUNKS, local, packed, 128), bf16),
            pltpu.VMEM((local, skeleton, columns), bf16),
            pltpu.VMEM(((n_pair - 1) * local, skeleton, columns), bf16),
            pltpu.VMEM((local, rows, skeleton), bf16),
            pltpu.VMEM((n_pair - 1, CHUNKS, rows, columns), bf16),
            pltpu.VMEM((n_pair - 1, CHUNKS, rows, columns), bf16),
            dma((6,)),
            dma,
            dma((CHUNKS,)),
            dma((CHUNKS,)),
            dma,
            dma,
            dma,
            dma,
        ],
        compiler_params=pltpu.CompilerParams(collective_id=0, has_side_effects=True, vmem_limit_bytes=VMEM),
    )(target, jnp.swapaxes(left, 2, 3), jnp.swapaxes(right, 2, 3), inverse, blocks, weights)
    return pl.pallas_call(
        store,
        name="store",
        out_shape=(
            jax.ShapeDtypeStruct(blocks.shape, f32),
            jax.ShapeDtypeStruct((skeleton, columns), f32),
        ),
        in_specs=[anywhere] * 2,
        out_specs=(anywhere, anywhere),
        scratch_shapes=[dma((2,))],
        compiler_params=pltpu.CompilerParams(vmem_limit_bytes=2**20),
    )(updated, panel)


def solution(mesh):
    in_specs = (
        P(("surf", "pair"), None, None, None),
        P(("surf", "pair"), None, None, None),
        P(("surf", "pair"), None, None),
        P(("surf", "pair"), None, None),
        P(("surf", "pair"), None, None),
        P("surf", None, "pair"),
    )
    out_specs = (P(("surf", "pair"), None, None), P("surf", "pair"))
    return jax.shard_map(body, mesh=mesh, in_specs=in_specs, out_specs=out_specs, check_vma=False)
```
